256 devices in a mesh: cells: 32 (over z, x), genes: 8 (over y, core).
Axes of the slice: x: 4, y: 4, z: 8, core: 2. Of those that a mesh axis runs over, the one named last changes fastest.
Arguments:
- expression: bfloat16 [131072, 4096], P('cells', 'genes'), may hold values from -200 to 200
- labels: int32 [131072], P('cells'), may hold values from 0 to 199, as said below
- loadings: bfloat16 [4096, 50], P('genes'), may hold values from -0.09375 to 0.09375
Outputs:
- adjusted: bfloat16 [131072, 4096], P('cells', 'genes')
- scores: float32 [131072, 50], P('cells')
The draws below stay inside these ranges and needn't reach their ends.
Inputs may be any that keep to these rules, and one draw needn't show every extreme that they name: `labels`: every batch has two or more cells.
All inputs are finite; a program needn't handle non-finite values.
Results may differ from the reference program's by a relative error of at most 0.0029.
Values sent between devices are 32-bit elements; how exact they have to be, the bound alone decides.
A program may use at most 64 MiB of HBM per device.

```python
import math
import jax
import jax.numpy as jnp
from jax import lax

GENES = 4096
BATCHES = 200
COMPONENTS = 50
SWEEPS = 10
CELLS = 131072


def label_table(key):
    rare_count = BATCHES // 3
    common_count = BATCHES - rare_count
    rare_top = max(2, min(30, CELLS // (2 * BATCHES)))
    keys = jax.random.split(jax.random.fold_in(key, 11), 5)
    order = jax.random.permutation(keys[0], BATCHES).astype(jnp.int32)
    rare_ids = order[:rare_count]
    common_ids = order[rare_count:]
    rare_sizes = jax.random.randint(keys[1], (rare_count,), 2, rare_top + 1, dtype=jnp.int32)
    rare_ends = jnp.cumsum(rare_sizes).astype(jnp.int32)
    rare_total = rare_ends[rare_count - 1]
    position = jnp.arange(CELLS, dtype=jnp.int32)
    rare_slot = jnp.minimum(jnp.searchsorted(rare_ends, position, side='right').astype(jnp.int32), rare_count - 1)
    base_slot = jnp.clip((position - rare_total) // 2, 0, common_count - 1).astype(jnp.int32)
    pick_first = jax.random.randint(keys[2], (CELLS,), 0, common_count, dtype=jnp.int32)
    pick_second = jax.random.randint(keys[3], (CELLS,), 0, common_count, dtype=jnp.int32)
    extra_slot = jnp.minimum(pick_first, pick_second)
    ordered = jnp.where(position < rare_total, rare_ids[rare_slot], jnp.where(position < rare_total + 2 * common_count, common_ids[base_slot], common_ids[extra_slot]))
    shuffle = jax.random.permutation(keys[4], CELLS).astype(jnp.int32)
    return ordered[shuffle].astype(jnp.int32)


def draw_labels(key, part):
    return label_table(key)


def draw_expression(key, part):
    labels = label_table(key)
    keys = jax.random.split(jax.random.fold_in(key, 23), 6)
    gene_scale = jnp.exp(jax.random.uniform(keys[0], (GENES,), jnp.float32, 0.0, jnp.log(10.0)))
    noise = jnp.clip(jax.random.normal(keys[4], (CELLS, GENES), jnp.float32), -5.0, 5.0)
    ramp_low = 0.5
    ramp_high = 3.0
    width_low = 0.2
    width_high = 0.8
    position = jnp.arange(GENES, dtype=jnp.float32) / (GENES - 1.0)
    gene_ramp = ramp_low + (ramp_high - ramp_low) * position
    gene_width = width_low + (width_high - width_low) * position
    gene_mean = jax.random.uniform(keys[1], (GENES,), jnp.float32, -2.0, 2.0)
    batch_offset = jax.random.uniform(keys[5], (BATCHES,), jnp.float32, -1.0, 1.0)
    shift = 0.4 * gene_ramp[None, :] * (jnp.clip(jax.random.normal(keys[2], (BATCHES, GENES), jnp.float32), -4.0, 4.0) + batch_offset[:, None])
    batch_scale = jnp.exp(jax.random.uniform(keys[3], (BATCHES, GENES), jnp.float32, -1.0, 1.0) * gene_width[None, :])
    values = gene_mean[None, :] + gene_scale[None, :] * (shift[labels] + batch_scale[labels] * noise) / 3.0
    return values.astype(jnp.bfloat16)


def shard_levels(rng, shape, pieces, least, largest):
    level, own = 1.0, jax.random.fold_in(rng, 6)
    for dim, shards_of in pieces:
        steps = jnp.exp(jax.random.uniform(jax.random.fold_in(own, dim), (shards_of,), jnp.float32, least / len(pieces), largest / len(pieces)))
        level = level * jnp.repeat(steps, shape[dim] // shards_of).reshape([-1 if axis == dim else 1 for axis in range(len(shape))])
    return level


def gaussian(own_key, shape, width, limit, cuts=(), kind=jnp.bfloat16):
    loudness = shard_levels(own_key, shape, cuts, -0.22, 0.18) if cuts else 1.0
    result = jax.random.normal(own_key, shape, jnp.float32) * width * loudness
    return jnp.minimum(jnp.maximum(result, -limit), limit).astype(kind)


def setup_inputs(seed: int = 0) -> dict:
    key_of = jax.random.split(jax.random.key(seed), 4)
    expression = draw_expression(jax.random.fold_in(key_of[3], 71), 0)
    labels = draw_labels(jax.random.fold_in(key_of[3], 71), 0)
    loadings = gaussian(key_of[2], (GENES, COMPONENTS), GENES ** -0.5, 0.09375, ((0, 8),))
    return {"expression": expression, "labels": labels, "loadings": loadings}


def batch_moments(sum_one, sum_two, counts, total_cells):
    grand = lax.optimization_barrier(jnp.sum(sum_one, axis=0)) / total_cells
    within = sum_two - sum_one * sum_one / counts[:, None]
    pooled = lax.optimization_barrier(jnp.sum(within, axis=0)) / total_cells + 1e-06
    gene_sd = jnp.sqrt(pooled)
    gamma_hat = (sum_one / counts[:, None] - grand[None, :]) / gene_sd[None, :]
    delta_hat = within / ((counts[:, None] - 1.0) * pooled[None, :])
    return (grand, gene_sd, gamma_hat, delta_hat)

def shrink(gamma_hat, delta_hat, counts):
    gamma_bar = lax.optimization_barrier(jnp.sum(gamma_hat, axis=1)) / GENES
    tau_sq = (lax.optimization_barrier(jnp.sum(gamma_hat * gamma_hat, axis=1)) - GENES * gamma_bar * gamma_bar) / (GENES - 1)
    delta_mean = lax.optimization_barrier(jnp.sum(delta_hat, axis=1)) / GENES
    delta_var = (lax.optimization_barrier(jnp.sum(delta_hat * delta_hat, axis=1)) - GENES * delta_mean * delta_mean) / (GENES - 1) + 1e-06
    a_prior = (2.0 * delta_var + delta_mean * delta_mean) / delta_var
    b_prior = (delta_mean * delta_var + delta_mean ** 3) / delta_var
    weight = counts[:, None]

    def sweep(sweep_index, state):
        gamma_now, delta_now = state
        gamma_next = (weight * tau_sq[:, None] * gamma_hat + delta_now * gamma_bar[:, None]) / (weight * tau_sq[:, None] + delta_now)
        sum_sq = (weight - 1.0) * delta_hat + weight * (gamma_hat - gamma_next) ** 2
        delta_next = (0.5 * sum_sq + b_prior[:, None]) / (0.5 * weight + a_prior[:, None] - 1.0)
        return (gamma_next, delta_next)
    gamma_star, delta_star = lax.fori_loop(0, SWEEPS, sweep, (gamma_hat, delta_hat))
    return (gamma_star, 1.0 / jnp.sqrt(delta_star))

def reference(expression, labels, loadings):
    block_rows = math.gcd(CELLS, 4096)
    block_count = CELLS // block_rows
    indices = jnp.arange(block_count, dtype=jnp.int32)

    def accumulate(totals, block_index):
        start = block_index * block_rows
        values = lax.dynamic_slice_in_dim(expression, start, block_rows, 0).astype(jnp.float32)
        local_labels = lax.dynamic_slice_in_dim(labels, start, block_rows, 0)
        first = jax.ops.segment_sum(values, local_labels, BATCHES)
        second = jax.ops.segment_sum(values * values, local_labels, BATCHES)
        number = jax.ops.segment_sum(jnp.ones((block_rows,), jnp.float32), local_labels, BATCHES)
        return ((totals[0] + first, totals[1] + second, totals[2] + number), None)
    zeros_table = jnp.zeros((BATCHES, GENES), jnp.float32)
    (sum_one, sum_two, counts), unused = lax.scan(accumulate, (zeros_table, zeros_table, jnp.zeros((BATCHES,), jnp.float32)), indices)
    grand, gene_sd, gamma_hat, delta_hat = batch_moments(sum_one, sum_two, counts, CELLS)
    gamma_star, scale_star = shrink(gamma_hat, delta_hat, counts)

    def adjust(block_index):
        start = block_index * block_rows
        values = lax.dynamic_slice_in_dim(expression, start, block_rows, 0).astype(jnp.float32)
        local_labels = lax.dynamic_slice_in_dim(labels, start, block_rows, 0)
        shifted = (values - grand[None, :]) / gene_sd[None, :]
        standard = (shifted - gamma_star[local_labels]) * scale_star[local_labels]
        adjusted = (gene_sd[None, :] * standard + grand[None, :]).astype(jnp.bfloat16)
        standard_low = standard.astype(jnp.bfloat16)
        partial_value = jnp.dot(standard_low, loadings, preferred_element_type=jnp.float32)
        return (adjusted, partial_value)
    adjusted, scores = lax.map(adjust, indices)
    return (adjusted.reshape(CELLS, GENES), scores.reshape(CELLS, COMPONENTS))
```

```python
import functools

import jax
import jax.numpy as jnp
from jax import lax
from jax.experimental import pallas as pl
from jax.experimental.pallas import tpu as pltpu
from jax.sharding import PartitionSpec as P

MESH = pl.DeviceIdType.MESH
GENES = 4096
BATCHES = 200
CELLS = 131072
SWEEPS = 10
COMPONENTS = 50

NZ, NX, NY = 8, 4, 4
ROWS, COLS = 4096, 512
LANES = 128
GROUPS = COLS // LANES
PART = 56
HALF = 32
STACK = NZ * PART
COUNT_ROW = 2 * BATCHES
PAD = 256
READ = 1024
STEP = 512
CHUNK_TOP = 32

f32, bf16, i32 = jnp.float32, jnp.bfloat16, jnp.int32
NT = (((1,), (1,)), ((), ()))


def z_offset(k):
    size = 4 - (k + 1) // 2
    return (size if k % 2 else NZ - size) % NZ


def remote(src, dst, send, recv, cells, genes):
    return pltpu.make_async_remote_copy(
        src_ref=src,
        dst_ref=dst,
        send_sem=send,
        recv_sem=recv,
        device_id={"cells": cells, "genes": genes},
        device_id_type=MESH,
    )


def kernel(
    labels,
    x_hbm,
    loadings_t,
    adjusted_hbm,
    scores_hbm,
    xv,
    outv,
    onehot,
    acc_one,
    acc_two,
    acc_count,
    sums,
    via_left,
    via_right,
    from_left,
    from_right,
    owned,
    from_z,
    table,
    terms,
    terms_y,
    terms_x,
    cols,
    gene_rows,
    wide,
    pair,
    part,
    part_recv,
    role,
    y_via_left,
    y_via_right,
    y_from_left,
    y_from_right,
    final,
    x_sem,
    out_sem,
    fin_sem,
    rs_send,
    rs_recv,
    z_send,
    z_recv,
    g_send,
    g_recv,
    ag_send,
    ag_recv,
    t_send,
    t_recv,
    d_send,
    d_recv,
    y_send,
    y_recv,
):
    me_c = lax.axis_index("cells")
    me_g = lax.axis_index("genes")
    mz, mx = lax.div(me_c, NX), lax.rem(me_c, NX)
    my, mh = lax.div(me_g, 2), lax.rem(me_g, 2)
    x_right, x_left, x_opp = (lax.rem(mx + d, NX) for d in (1, 3, 2))
    y_right, y_left, y_opp = (lax.rem(my + d, NY) for d in (1, 3, 2))

    def cell(z, x):
        return z * NX + x

    right, left = cell(mz, x_right), cell(mz, x_left)
    barrier = pltpu.get_barrier_semaphore()

    def greet(c, g):
        pl.semaphore_signal(
            barrier, inc=1, device_id={"cells": c, "genes": g}, device_id_type=MESH
        )

    for r in range(1, NX):
        greet(cell(mz, lax.rem(mx + r, NX)), me_g)
    for r in range(1, NZ):
        greet(cell(lax.rem(mz + r, NZ), mx), me_g)
    for r in range(1, 2 * NY):
        greet(me_c, lax.rem(me_g + r, 2 * NY))

    def x_copy(i):
        rows = pl.ds(pl.multiple_of(i * READ, READ), READ)
        return pltpu.make_async_copy(x_hbm.at[rows, :], xv.at[rows, :], x_sem.at[i])

    for i in range(ROWS // READ):
        x_copy(i).start()
    acc_one[...] = jnp.zeros_like(acc_one)
    acc_two[...] = jnp.zeros_like(acc_two)
    acc_count[...] = jnp.zeros_like(acc_count)

    def first_pass(i, carry):
        tile = labels[pl.ds(pl.multiple_of(i * 8, 8), 8), :]
        ids = lax.broadcasted_iota(i32, (208, LANES), 0)
        members = jnp.concatenate(
            [jnp.where(ids == tile[j : j + 1, :], 1.0, 0.0).astype(bf16) for j in range(8)], axis=1
        )
        x_copy(i).wait()
        values = xv[pl.ds(pl.multiple_of(i * READ, READ), READ), :]
        widened = values.astype(f32)
        square = widened * widened
        upper = square.astype(bf16)
        lower = (square - upper.astype(f32)).astype(bf16)
        acc_one[...] += jnp.dot(members, values, preferred_element_type=f32)
        acc_two[...] += jnp.dot(members, upper, preferred_element_type=f32) + jnp.dot(
            members, lower, preferred_element_type=f32
        )
        ones = jnp.ones((8, READ), bf16)
        acc_count[:, :208] += lax.dot_general(ones, members, NT, preferred_element_type=f32)
        return carry

    lax.fori_loop(0, ROWS // READ, first_pass, 0)
    sub = lax.broadcasted_iota(i32, (8, LANES), 0)
    count_tile = jnp.where(sub == 0, acc_count[:, :LANES], acc_count[:, LANES:])
    for g in range(GROUPS):
        lanes = slice(g * LANES, (g + 1) * LANES)
        sums[g, 0:BATCHES, :] = acc_one[0:BATCHES, lanes]
        sums[g, BATCHES:COUNT_ROW, :] = acc_two[0:BATCHES, lanes]
        sums[g, COUNT_ROW : COUNT_ROW + 8, :] = count_tile
        sums[g, COUNT_ROW + 8 :, :] = jnp.zeros((STACK - COUNT_ROW - 8, LANES), f32)

    pl.semaphore_wait(barrier, NX - 1 + NZ - 1 + 2 * NY - 1)

    def z_of(k):
        return lax.rem(mz + z_offset(k), NZ)

    def top(z):
        return pl.ds(pl.multiple_of(z * PART, 8), HALF)

    def low(z):
        return pl.ds(pl.multiple_of(z * PART + HALF, 8), PART - HALF)

    def whole(z):
        return pl.ds(pl.multiple_of(z * PART, 8), PART)

    def rs(kind, k):
        z = z_of(k)
        src, dst, to = (
            (sums.at[x_opp, top(z)], via_left.at[k], right),
            (sums.at[x_opp, low(z)], via_right.at[k], left),
            (sums.at[x_right, low(z)], from_left.at[k, HALF:PART], right),
            (sums.at[x_left, top(z)], from_right.at[k, 0:HALF], left),
            (sums.at[x_right, top(z)], from_left.at[k, 0:HALF], right),
            (sums.at[x_left, low(z)], from_right.at[k, HALF:PART], left),
        )[kind]
        return remote(src, dst, rs_send.at[kind, k], rs_recv.at[kind, k], to, me_g)

    def z_copy(k):
        return remote(owned.at[k], from_z.at[k], z_send.at[k], z_recv.at[k], cell(z_of(k), mx), me_g)

    def issue(k):
        for kind in range(4):
            rs(kind, k).start()

    def merge(k):
        z = z_of(k)
        rs(0, k).wait_recv()
        sums[x_right, top(z)] += via_left[k]
        rs(4, k).start()
        rs(1, k).wait_recv()
        sums[x_left, low(z)] += via_right[k]
        rs(5, k).start()

    def finish(k):
        for kind in range(2, 6):
            rs(kind, k).wait_recv()
        owned[k] = sums[mx, whole(z_of(k))] + from_left[k] + from_right[k]
        if k < NZ - 1:
            z_copy(k).start()

    issue(0)
    issue(1)

    def spread_labels(i, carry):
        wide_labels = jnp.broadcast_to(labels[pl.ds(i, 1), :].astype(f32), (LANES, LANES)).T
        ids = lax.broadcasted_iota(i32, (LANES, LANES), 1).astype(f32)
        rows = pl.ds(pl.multiple_of(i * LANES, LANES), LANES)
        onehot[rows, 0:LANES] = jnp.where(wide_labels == ids, 1.0, 0.0).astype(bf16)
        onehot[rows, LANES:PAD] = jnp.where(wide_labels == ids + LANES, 1.0, 0.0).astype(bf16)
        return carry

    lax.fori_loop(0, ROWS // LANES, spread_labels, 0)
    for k in range(NZ):
        merge(k)
        if k + 2 < NZ:
            issue(k + 2)
        if k >= 1:
            finish(k - 1)
    finish(NZ - 1)
    total = owned[NZ - 1]
    for k in range(NZ - 1):
        z_copy(k).wait_recv()
        total = total + from_z[k]
    table[mx, whole(mz)] = total

    def g_copy(k):
        spot = table.at[mx, whole(mz)]
        return remote(spot, spot, g_send.at[k], g_recv.at[k], cell(z_of(k), mx), me_g)

    def ag(kind, k):
        z = lax.rem(mz + NZ - z_offset(k), NZ)
        spot, to = (
            (table.at[mx, whole(z)], right),
            (table.at[mx, whole(z)], left),
            (table.at[x_left, top(z)], right),
            (table.at[x_right, low(z)], left),
        )[kind]
        return remote(spot, spot, ag_send.at[kind, k], ag_recv.at[kind, k], to, me_g)

    for k in range(NZ - 1):
        g_copy(k).start()
    order = (7, 5, 6, 3, 4, 1, 2, 0)

    def pass_on(k):
        ag(0, k).wait_recv()
        ag(2, k).start()
        ag(1, k).wait_recv()
        ag(3, k).start()

    for spot, k in enumerate(order):
        if k != NZ - 1:
            g_copy(k).wait_recv()
        ag(0, k).start()
        ag(1, k).start()
        if spot >= 1:
            pass_on(order[spot - 1])

    def column(row):
        return jnp.broadcast_to(row, (LANES, PAD)).T

    counts = jnp.concatenate(
        [table[mx, COUNT_ROW : COUNT_ROW + 1, :], table[mx, COUNT_ROW + 1 : COUNT_ROW + 2, :]], axis=1
    )
    weight = column(counts)
    cols[0] = weight
    cols[1] = 1.0 / weight
    cols[2] = 1.0 / (weight - 1.0)

    def gene_stats(g):
        one, two = table[g, 0:BATCHES, :], table[g, BATCHES:COUNT_ROW, :]
        share = cols[1, 0:BATCHES, :]
        grand = jnp.sum(one, axis=0, keepdims=True) / CELLS
        mean = one * share
        within = two - one * mean
        pooled = jnp.sum(within, axis=0, keepdims=True) / CELLS + 1e-06
        return mean, within, grand, pooled

    mean, within, grand, pooled = gene_stats(mx)
    gamma_hat = (mean - grand) / jnp.sqrt(pooled)
    delta_hat = within * cols[2, 0:BATCHES, :] / pooled
    spare = jnp.zeros((PAD - BATCHES, LANES), f32)

    def over_genes(v):
        return lax.dot_general(
            jnp.ones((8, LANES), f32),
            jnp.concatenate([v, spare], axis=0),
            NT,
            precision=lax.Precision.HIGHEST,
            preferred_element_type=f32,
        )

    sub_wide = lax.broadcasted_iota(i32, (8, PAD), 0)
    t0, t1 = over_genes(gamma_hat), over_genes(gamma_hat * gamma_hat)
    t2, t3 = over_genes(delta_hat), over_genes(delta_hat * delta_hat)
    terms[0] = jnp.where(sub_wide == 0, t0, jnp.where(sub_wide == 1, t1, jnp.where(sub_wide == 2, t2, t3)))

    def terms_over_y(r):
        return remote(
            terms.at[0], terms_y.at[r], t_send.at[0, r], t_recv.at[0, r], me_c, lax.rem(me_g + r, 2 * NY)
        )

    def terms_over_x(r):
        return remote(
            terms.at[1],
            terms_x.at[r],
            t_send.at[1, r],
            t_recv.at[1, r],
            cell(mz, lax.rem(mx + r, NX)),
            me_g,
        )

    for r in range(1, 2 * NY):
        terms_over_y(r).start()
    pass_on(order[-1])
    running = terms[0]
    for r in range(1, 2 * NY):
        terms_over_y(r).wait_recv()
        running = running + terms_y[r]
    terms[1] = running
    for r in range(1, NX):
        terms_over_x(r).start()
    for k in order:
        ag(2, k).wait_recv()
        ag(3, k).wait_recv()
    for g in range(GROUPS):
        mean, within, grand, pooled = gene_stats(g)
        gene_rows[0:1, g * LANES : (g + 1) * LANES] = grand
        gene_rows[1:2, g * LANES : (g + 1) * LANES] = jnp.sqrt(pooled)
        gene_rows[2:3, g * LANES : (g + 1) * LANES] = 1.0 / jnp.sqrt(pooled)
        gene_rows[3:4, g * LANES : (g + 1) * LANES] = 1.0 / pooled
    for r in range(1, NX):
        terms_over_x(r).wait_recv()
        running = running + terms_x[r]
    gamma_bar = running[0:1, :] / GENES
    tau_sq = (running[1:2, :] - GENES * gamma_bar * gamma_bar) / (GENES - 1)
    delta_mean = running[2:3, :] / GENES
    delta_var = (running[3:4, :] - GENES * delta_mean * delta_mean) / (GENES - 1) + 1e-06
    a_prior = (2.0 * delta_var + delta_mean * delta_mean) / delta_var
    b_prior = (delta_mean * delta_var + delta_mean * delta_mean * delta_mean) / delta_var
    cols[3] = column(counts * tau_sq)
    cols[4] = column(gamma_bar)
    cols[5] = column(1.0 / (0.5 * counts + a_prior - 1.0))
    cols[6] = column(b_prior)

    block = 40

    def shrink(i, carry):
        start = pl.multiple_of(i * block, 8)
        rows = pl.ds(start, block)
        weight, share, share_less = cols[0, rows], cols[1, rows], cols[2, rows]
        pull, centre, inverse, prior = cols[3, rows], cols[4, rows], cols[5, rows], cols[6, rows]
        slope = 0.5 * weight * inverse
        hats, leans, floors, deltas = [], [], [], []
        for g in range(GROUPS):
            lanes = slice(g * LANES, (g + 1) * LANES)
            one = table[g, rows, :]
            two = table[g, pl.ds(pl.multiple_of(start + BATCHES, 8), block), :]
            mean = one * share
            hat = (mean - gene_rows[0:1, lanes]) * gene_rows[2:3, lanes]
            delta = (two - one * mean) * share_less * gene_rows[3:4, lanes]
            hats.append(hat)
            leans.append(hat - centre)
            floors.append((0.5 * (weight - 1.0) * delta + prior) * inverse)
            deltas.append(delta)
        moves = [None] * GROUPS
        for _ in range(SWEEPS):
            for g in range(GROUPS):
                moves[g] = deltas[g] * leans[g] / (pull + deltas[g])
                deltas[g] = floors[g] + slope * (moves[g] * moves[g])
        for g in range(GROUPS):
            lanes = slice(g * LANES, (g + 1) * LANES)
            scale = lax.rsqrt(deltas[g])
            wide[0, rows, lanes] = scale * gene_rows[2:3, lanes]
            wide[1, rows, lanes] = (hats[g] - moves[g]) * scale
        return carry

    lax.fori_loop(0, BATCHES // block, shrink, 0)
    wide[:, BATCHES:PAD, :] = jnp.zeros((2, PAD - BATCHES, COLS), f32)
    for g in range(2):
        for side in range(2):
            value = wide[side, :, g * PAD : (g + 1) * PAD]
            upper = value.astype(bf16)
            at = slice((2 * g + side) * PAD, (2 * g + side + 1) * PAD)
            pair[0:PAD, at] = upper
            pair[PAD : 2 * PAD, at] = (value - upper.astype(f32)).astype(bf16)

    other = 1 - mh
    partner = my * 2 + other
    to_right, to_left = y_right * 2 + mh, y_left * 2 + mh
    upper_rows, lower_rows = slice(0, CHUNK_TOP), slice(CHUNK_TOP, COMPONENTS)

    def y_at(i):
        step = jnp.where(i == 0, 2, jnp.where(i == 1, 1, jnp.where(i == 2, 3, 0)))
        return lax.rem(my + step, NY)

    def swap(i):
        return remote(part.at[i], part_recv.at[i], d_send.at[i], d_recv.at[i], me_c, partner)

    def y_copy(kind):
        src, dst, to = (
            (role.at[0, upper_rows], y_via_left, to_right),
            (role.at[0, lower_rows], y_via_right, to_left),
            (role.at[1, lower_rows], y_from_left.at[lower_rows], to_right),
            (role.at[2, upper_rows], y_from_right.at[upper_rows], to_left),
            (role.at[1, upper_rows], y_from_left.at[upper_rows], to_right),
            (role.at[2, lower_rows], y_from_right.at[lower_rows], to_left),
        )[kind]
        return remote(src, dst, y_send.at[kind], y_recv.at[kind], me_c, to)

    def adjust(i, carry):
        mine = i >= NY
        place = jnp.where(mine, i - NY, i)
        chunk = jnp.where(mine, mh, other) * NY + y_at(place)
        rows = pl.ds(pl.multiple_of(chunk * STEP, STEP), STEP)
        members = onehot[rows, :]
        members = jnp.concatenate([members, members], axis=1)
        lows = []
        for g in range(2):
            lanes = slice(g * PAD, (g + 1) * PAD)
            found = jnp.dot(members, pair[:, 2 * g * PAD : 2 * (g + 1) * PAD], preferred_element_type=f32)
            grand, gene_sd = gene_rows[0:1, lanes], gene_rows[1:2, lanes]
            standard = (xv[rows, lanes].astype(f32) - grand) * found[:, :PAD] - found[:, PAD:]
            outv[rows, lanes] = (gene_sd * standard + grand).astype(bf16)
            lows.append(standard.astype(bf16))
        out_copy(i, rows).start()
        part[i] = lax.dot_general(
            loadings_t[...], jnp.concatenate(lows, axis=1), NT, preferred_element_type=f32
        )

        @pl.when(i < NY)
        def _():
            swap(i).start()

        @pl.when(mine)
        def _():
            swap(place).wait_recv()
            role[place] = part[i] + part_recv[place]

        @pl.when(i == NY)
        def _():
            y_copy(0).start()
            y_copy(1).start()

        @pl.when(i == NY + 1)
        def _():
            y_copy(2).start()

        @pl.when(i == NY + 2)
        def _():
            y_copy(3).start()
            y_copy(0).wait_recv()
            role[1, upper_rows] += y_via_left[...]
            y_copy(4).start()
            y_copy(1).wait_recv()
            role[2, lower_rows] += y_via_right[...]
            y_copy(5).start()

        return carry

    def out_copy(i, rows):
        return pltpu.make_async_copy(outv.at[rows, :], adjusted_hbm.at[rows, :], out_sem.at[i])

    lax.fori_loop(0, 2 * NY, adjust, 0)
    for kind in range(2, 6):
        y_copy(kind).wait_recv()
    mine = mh * NY
    final[mine + my] = role[3] + y_from_left[...] + y_from_right[...]

    def y_gather(kind):
        spot, to = (
            (final.at[mine + my, upper_rows], to_right),
            (final.at[mine + my, lower_rows], to_left),
            (final.at[mine + my, lower_rows], to_right),
            (final.at[mine + my, upper_rows], to_left),
            (final.at[mine + y_left, upper_rows], to_right),
            (final.at[mine + y_right, lower_rows], to_left),
        )[kind]
        return remote(spot, spot, y_send.at[6 + kind], y_recv.at[6 + kind], me_c, to)

    def share(i, y):
        spot = final.at[mine + y]
        return remote(spot, spot, d_send.at[NY + i], d_recv.at[NY + i], me_c, partner)

    def store(i, chunk):
        return pltpu.make_async_copy(
            final.at[chunk],
            scores_hbm.at[:, pl.ds(pl.multiple_of(chunk * STEP, STEP), STEP)],
            fin_sem.at[i],
        )

    for kind in range(4):
        y_gather(kind).start()
    share(0, my).start()
    store(0, mine + my).start()
    y_gather(0).wait_recv()
    y_gather(4).start()
    y_gather(1).wait_recv()
    y_gather(5).start()
    y_gather(2).wait_recv()
    share(1, y_left).start()
    store(1, mine + y_left).start()
    y_gather(3).wait_recv()
    share(2, y_right).start()
    store(2, mine + y_right).start()
    y_gather(4).wait_recv()
    y_gather(5).wait_recv()
    share(3, y_opp).start()
    store(3, mine + y_opp).start()
    for i, y in enumerate((my, y_left, y_right, y_opp)):
        share(i, y).wait_recv()
        store(NY + i, other * NY + y).start()

    for k in range(NZ):
        for kind in range(6):
            rs(kind, k).wait_send()
        for kind in range(4):
            ag(kind, k).wait_send()
        if k < NZ - 1:
            z_copy(k).wait_send()
            g_copy(k).wait_send()
    for r in range(1, 2 * NY):
        terms_over_y(r).wait_send()
    for r in range(1, NX):
        terms_over_x(r).wait_send()
    for i in range(NY):
        swap(i).wait_send()
    for kind in range(6):
        y_copy(kind).wait_send()
        y_gather(kind).wait_send()
    for i, y in enumerate((my, y_left, y_right, y_opp)):
        share(i, y).wait_send()
        store(i, mine + y).wait()
        store(NY + i, other * NY + y).wait()
    for i in range(2 * NY):
        out_copy(i, pl.ds(i * STEP, STEP)).wait()


def body(expression, labels, loadings):
    dma = pltpu.SemaphoreType.DMA
    vmem = pltpu.VMEM
    adjusted, scores_t = pl.pallas_call(
        kernel,
        out_shape=(
            jax.ShapeDtypeStruct((ROWS, COLS), bf16),
            jax.ShapeDtypeStruct((COMPONENTS, ROWS), f32),
        ),
        in_specs=[
            pl.BlockSpec(memory_space=vmem),
            pl.BlockSpec(memory_space=pl.ANY),
            pl.BlockSpec(memory_space=vmem),
        ],
        out_specs=(pl.BlockSpec(memory_space=pl.ANY), pl.BlockSpec(memory_space=pl.ANY)),
        scratch_shapes=[
            vmem((ROWS, COLS), bf16),
            vmem((ROWS, COLS), bf16),
            vmem((ROWS, PAD), bf16),
            vmem((208, COLS), f32),
            vmem((208, COLS), f32),
            vmem((8, PAD), f32),
            vmem((GROUPS, STACK, LANES), f32),
            vmem((NZ, HALF, LANES), f32),
            vmem((NZ, PART - HALF, LANES), f32),
            vmem((NZ, PART, LANES), f32),
            vmem((NZ, PART, LANES), f32),
            vmem((NZ, PART, LANES), f32),
            vmem((NZ, PART, LANES), f32),
            vmem((GROUPS, STACK, LANES), f32),
            vmem((2, 8, PAD), f32),
            vmem((2 * NY, 8, PAD), f32),
            vmem((NX, 8, PAD), f32),
            vmem((7, PAD, LANES), f32),
            vmem((8, COLS), f32),
            vmem((2, PAD, COLS), f32),
            vmem((2 * PAD, 2 * COLS), bf16),
            vmem((2 * NY, COMPONENTS, STEP), f32),
            vmem((NY, COMPONENTS, STEP), f32),
            vmem((NY, COMPONENTS, STEP), f32),
            vmem((CHUNK_TOP, STEP), f32),
            vmem((COMPONENTS - CHUNK_TOP, STEP), f32),
            vmem((COMPONENTS, STEP), f32),
            vmem((COMPONENTS, STEP), f32),
            vmem((2 * NY, COMPONENTS, STEP), f32),
            dma((ROWS // READ,)),
            dma((2 * NY,)),
            dma((2 * NY,)),
            dma((6, NZ)),
            dma((6, NZ)),
            dma((NZ - 1,)),
            dma((NZ - 1,)),
            dma((NZ - 1,)),
            dma((NZ - 1,)),
            dma((4, NZ)),
            dma((4, NZ)),
            dma((2, 2 * NY)),
            dma((2, 2 * NY)),
            dma((2 * NY,)),
            dma((2 * NY,)),
            dma((12,)),
            dma((12,)),
        ],
        compiler_params=pltpu.CompilerParams(
            collective_id=0, has_side_effects=True, vmem_limit_bytes=56 * 1024 * 1024
        ),
        name="combat",
    )(labels.reshape(ROWS // LANES, LANES), expression, loadings.T)
    return adjusted, scores_t.T


def solution(mesh):
    return jax.shard_map(
        body,
        mesh=mesh,
        in_specs=(P("cells", "genes"), P("cells"), P("genes", None)),
        out_specs=(P("cells", "genes"), P("cells", None)),
        check_vma=False,
    )
```

```python
import functools

import jax
import jax.numpy as jnp
from jax import lax
from jax.experimental import pallas as pl
from jax.experimental.pallas import tpu as pltpu
from jax.sharding import PartitionSpec as P

MESH = pl.DeviceIdType.MESH
GENES = 4096
BATCHES = 200
CELLS = 131072
SWEEPS = 10
COMPONENTS = 50

NZ, NX, NY = 8, 4, 4
ROWS, COLS = 4096, 512
LANES = 128
GROUPS = COLS // LANES
PART = 56
HALF = 32
STACK = NZ * PART
COUNT_ROW = 2 * BATCHES
PAD = 256
READ = 1024
STEP = 512
LAG = 3
GATHER_LAG = 5
CHUNK_TOP = 32

f32, bf16, i32 = jnp.float32, jnp.bfloat16, jnp.int32
NT = (((1,), (1,)), ((), ()))


def z_offset(k):
    size = 4 - (k + 1) // 2
    return (size if k % 2 else NZ - size) % NZ


def remote(src, dst, send, recv, cells, genes):
    return pltpu.make_async_remote_copy(
        src_ref=src,
        dst_ref=dst,
        send_sem=send,
        recv_sem=recv,
        device_id={"cells": cells, "genes": genes},
        device_id_type=MESH,
    )


def kernel(
    labels,
    x_hbm,
    loadings_t,
    outv,
    scores_out,
    xv,
    onehot,
    acc_one,
    acc_two,
    acc_count,
    sums,
    via_left,
    via_right,
    from_left,
    from_right,
    owned,
    from_z,
    table,
    terms,
    terms_y,
    terms_x,
    cols,
    gene_rows,
    wide,
    pair,
    part,
    part_recv,
    role,
    y_via_left,
    y_via_right,
    y_from_left,
    y_from_right,
    final,
    x_sem,
    rs_send,
    rs_recv,
    z_send,
    z_recv,
    g_send,
    g_recv,
    ag_send,
    ag_recv,
    t_send,
    t_recv,
    d_send,
    d_recv,
    y_send,
    y_recv,
):
    me_c = lax.axis_index("cells")
    me_g = lax.axis_index("genes")
    mz, mx = lax.div(me_c, NX), lax.rem(me_c, NX)
    my, mh = lax.div(me_g, 2), lax.rem(me_g, 2)
    x_right, x_left, x_opp = (lax.rem(mx + d, NX) for d in (1, 3, 2))
    y_right, y_left, y_opp = (lax.rem(my + d, NY) for d in (1, 3, 2))

    def cell(z, x):
        return z * NX + x

    right, left = cell(mz, x_right), cell(mz, x_left)
    barrier = pltpu.get_barrier_semaphore()

    def greet(c, g):
        pl.semaphore_signal(
            barrier, inc=1, device_id={"cells": c, "genes": g}, device_id_type=MESH
        )

    for r in range(1, NX):
        greet(cell(mz, lax.rem(mx + r, NX)), me_g)
    for r in range(1, NZ):
        greet(cell(lax.rem(mz + r, NZ), mx), me_g)
    for r in range(1, 2 * NY):
        greet(me_c, lax.rem(me_g + r, 2 * NY))

    def x_copy(i):
        rows = pl.ds(pl.multiple_of(i * READ, READ), READ)
        return pltpu.make_async_copy(x_hbm.at[rows, :], xv.at[rows, :], x_sem.at[i])

    for i in range(ROWS // READ):
        x_copy(i).start()
    acc_one[...] = jnp.zeros_like(acc_one)
    acc_two[...] = jnp.zeros_like(acc_two)
    acc_count[...] = jnp.zeros_like(acc_count)

    def first_pass(i, carry):
        tile = labels[pl.ds(pl.multiple_of(i * 8, 8), 8), :]
        ids = lax.broadcasted_iota(i32, (208, LANES), 0)
        members = jnp.concatenate(
            [jnp.where(ids == tile[j : j + 1, :], 1.0, 0.0).astype(bf16) for j in range(8)], axis=1
        )
        x_copy(i).wait()
        values = xv[pl.ds(pl.multiple_of(i * READ, READ), READ), :]
        widened = values.astype(f32)
        square = widened * widened
        upper = square.astype(bf16)
        lower = (square - upper.astype(f32)).astype(bf16)
        acc_one[...] += jnp.dot(members, values, preferred_element_type=f32)
        acc_two[...] += jnp.dot(members, upper, preferred_element_type=f32) + jnp.dot(
            members, lower, preferred_element_type=f32
        )
        ones = jnp.ones((8, READ), bf16)
        acc_count[:, :208] += lax.dot_general(ones, members, NT, preferred_element_type=f32)
        return carry

    lax.fori_loop(0, ROWS // READ, first_pass, 0)
    sub = lax.broadcasted_iota(i32, (8, LANES), 0)
    count_tile = jnp.where(sub == 0, acc_count[:, :LANES], acc_count[:, LANES:])
    for g in range(GROUPS):
        lanes = slice(g * LANES, (g + 1) * LANES)
        sums[g, 0:BATCHES, :] = acc_one[0:BATCHES, lanes]
        sums[g, BATCHES:COUNT_ROW, :] = acc_two[0:BATCHES, lanes]
        sums[g, COUNT_ROW : COUNT_ROW + 8, :] = count_tile
        sums[g, COUNT_ROW + 8 :, :] = jnp.zeros((STACK - COUNT_ROW - 8, LANES), f32)

    pl.semaphore_wait(barrier, NX - 1 + NZ - 1 + 2 * NY - 1)

    def z_of(k):
        return lax.rem(mz + z_offset(k), NZ)

    def top(z):
        return pl.ds(pl.multiple_of(z * PART, 8), HALF)

    def low(z):
        return pl.ds(pl.multiple_of(z * PART + HALF, 8), PART - HALF)

    def whole(z):
        return pl.ds(pl.multiple_of(z * PART, 8), PART)

    def rs(kind, k):
        z = z_of(k)
        src, dst, to = (
            (sums.at[x_opp, top(z)], via_left.at[k], right),
            (sums.at[x_opp, low(z)], via_right.at[k], left),
            (sums.at[x_right, low(z)], from_left.at[k, HALF:PART], right),
            (sums.at[x_left, top(z)], from_right.at[k, 0:HALF], left),
            (sums.at[x_right, top(z)], from_left.at[k, 0:HALF], right),
            (sums.at[x_left, low(z)], from_right.at[k, HALF:PART], left),
        )[kind]
        return remote(src, dst, rs_send.at[kind, k], rs_recv.at[kind, k], to, me_g)

    def z_copy(k):
        return remote(owned.at[k], from_z.at[k], z_send.at[k], z_recv.at[k], cell(z_of(k), mx), me_g)

    def merge(k):
        z = z_of(k)
        rs(0, k).wait_recv()
        sums[x_right, top(z)] += via_left[k]
        rs(4, k).start()
        rs(1, k).wait_recv()
        sums[x_left, low(z)] += via_right[k]
        rs(5, k).start()
        rs(2, k).start()
        rs(3, k).start()

    def finish(k):
        for kind in range(2, 6):
            rs(kind, k).wait_recv()
        owned[k] = sums[mx, whole(z_of(k))] + from_left[k] + from_right[k]
        if k < NZ - 1:
            z_copy(k).start()

    for k in range(NZ):
        rs(0, k).start()
        rs(1, k).start()

    def spread_labels(i, carry):
        tile = labels[pl.ds(pl.multiple_of(i * 8, 8), 8), :].astype(f32)
        ids = lax.broadcasted_iota(i32, (LANES, LANES), 1).astype(f32)
        for j in range(8):
            wide_labels = jnp.broadcast_to(tile[j : j + 1, :], (LANES, LANES)).T
            rows = pl.ds(pl.multiple_of(i * 8 * LANES + j * LANES, LANES), LANES)
            onehot[rows, 0:LANES] = jnp.where(wide_labels == ids, 1.0, 0.0).astype(bf16)
            onehot[rows, LANES:PAD] = jnp.where(wide_labels == ids + LANES, 1.0, 0.0).astype(bf16)
        return carry

    half_labels = ROWS // (16 * LANES)
    lax.fori_loop(0, half_labels, spread_labels, 0)
    for k in range(NZ + LAG):
        if k < NZ:
            merge(k)
        if k >= LAG:
            finish(k - LAG)
    total = owned[NZ - 1]
    for k in range(NZ - 1):
        z_copy(k).wait_recv()
        total = total + from_z[k]
    table[mx, whole(mz)] = total

    def g_copy(k):
        spot = table.at[mx, whole(mz)]
        return remote(spot, spot, g_send.at[k], g_recv.at[k], cell(z_of(k), mx), me_g)

    def ag(kind, k):
        z = lax.rem(mz + NZ - z_offset(k), NZ)
        spot, to = (
            (table.at[mx, whole(z)], right),
            (table.at[mx, whole(z)], left),
            (table.at[x_left, top(z)], right),
            (table.at[x_right, low(z)], left),
        )[kind]
        return remote(spot, spot, ag_send.at[kind, k], ag_recv.at[kind, k], to, me_g)

    order = (7, 5, 6, 3, 4, 1, 2, 0)
    for k in order[1:]:
        g_copy(k).start()

    def pass_on(k):
        ag(0, k).wait_recv()
        ag(2, k).start()
        ag(1, k).wait_recv()
        ag(3, k).start()

    for spot, k in enumerate(order):
        if k != NZ - 1:
            g_copy(k).wait_recv()
        ag(0, k).start()
        ag(1, k).start()
        if spot == 0:
            lax.fori_loop(half_labels, 2 * half_labels, spread_labels, 0)
        if spot >= GATHER_LAG:
            pass_on(order[spot - GATHER_LAG])

    def column(row):
        return jnp.broadcast_to(row, (LANES, PAD)).T

    counts = jnp.concatenate(
        [table[mx, COUNT_ROW : COUNT_ROW + 1, :], table[mx, COUNT_ROW + 1 : COUNT_ROW + 2, :]], axis=1
    )
    weight = column(counts)
    cols[0] = weight
    cols[1] = 1.0 / weight
    cols[2] = 1.0 / (weight - 1.0)

    def gene_stats(g):
        one, two = table[g, 0:BATCHES, :], table[g, BATCHES:COUNT_ROW, :]
        share = cols[1, 0:BATCHES, :]
        grand = jnp.sum(one, axis=0, keepdims=True) / CELLS
        mean = one * share
        within = two - one * mean
        pooled = jnp.sum(within, axis=0, keepdims=True) / CELLS + 1e-06
        return mean, within, grand, pooled

    mean, within, grand, pooled = gene_stats(mx)
    gamma_hat = (mean - grand) / jnp.sqrt(pooled)
    delta_hat = within * cols[2, 0:BATCHES, :] / pooled
    spare = jnp.zeros((PAD - BATCHES, LANES), f32)

    def over_genes(v):
        return lax.dot_general(
            jnp.ones((8, LANES), f32),
            jnp.concatenate([v, spare], axis=0),
            NT,
            precision=lax.Precision.HIGHEST,
            preferred_element_type=f32,
        )

    sub_wide = lax.broadcasted_iota(i32, (8, PAD), 0)
    t0, t1 = over_genes(gamma_hat), over_genes(gamma_hat * gamma_hat)
    t2, t3 = over_genes(delta_hat), over_genes(delta_hat * delta_hat)
    terms[0] = jnp.where(sub_wide == 0, t0, jnp.where(sub_wide == 1, t1, jnp.where(sub_wide == 2, t2, t3)))

    def terms_over_y(r):
        return remote(
            terms.at[0], terms_y.at[r], t_send.at[0, r], t_recv.at[0, r], me_c, lax.rem(me_g + r, 2 * NY)
        )

    def terms_over_x(r):
        return remote(
            terms.at[1],
            terms_x.at[r],
            t_send.at[1, r],
            t_recv.at[1, r],
            cell(mz, lax.rem(mx + r, NX)),
            me_g,
        )

    for r in range(1, 2 * NY):
        terms_over_y(r).start()
    for k in order[NZ - GATHER_LAG :]:
        pass_on(k)
    running = terms[0]
    for r in range(1, 2 * NY):
        terms_over_y(r).wait_recv()
        running = running + terms_y[r]
    terms[1] = running
    for r in range(1, NX):
        terms_over_x(r).start()
    for k in order:
        ag(2, k).wait_recv()
        ag(3, k).wait_recv()
    for g in range(GROUPS):
        mean, within, grand, pooled = gene_stats(g)
        gene_rows[0:1, g * LANES : (g + 1) * LANES] = grand
        gene_rows[1:2, g * LANES : (g + 1) * LANES] = jnp.sqrt(pooled)
        gene_rows[2:3, g * LANES : (g + 1) * LANES] = 1.0 / jnp.sqrt(pooled)
        gene_rows[3:4, g * LANES : (g + 1) * LANES] = 1.0 / pooled
    for r in range(1, NX):
        terms_over_x(r).wait_recv()
        running = running + terms_x[r]
    gamma_bar = running[0:1, :] / GENES
    tau_sq = (running[1:2, :] - GENES * gamma_bar * gamma_bar) / (GENES - 1)
    delta_mean = running[2:3, :] / GENES
    delta_var = (running[3:4, :] - GENES * delta_mean * delta_mean) / (GENES - 1) + 1e-06
    a_prior = (2.0 * delta_var + delta_mean * delta_mean) / delta_var
    b_prior = (delta_mean * delta_var + delta_mean * delta_mean * delta_mean) / delta_var
    cols[3] = column(counts * tau_sq)
    cols[4] = column(gamma_bar)
    cols[5] = column(1.0 / (0.5 * counts + a_prior - 1.0))
    cols[6] = column(b_prior)

    block = 40

    def shrink(i, carry):
        start = pl.multiple_of(i * block, 8)
        rows = pl.ds(start, block)
        weight, share, share_less = cols[0, rows], cols[1, rows], cols[2, rows]
        pull, centre, inverse, prior = cols[3, rows], cols[4, rows], cols[5, rows], cols[6, rows]
        slope = 0.5 * weight * inverse
        hats, leans, floors, deltas = [], [], [], []
        for g in range(GROUPS):
            lanes = slice(g * LANES, (g + 1) * LANES)
            one = table[g, rows, :]
            two = table[g, pl.ds(pl.multiple_of(start + BATCHES, 8), block), :]
            mean = one * share
            hat = (mean - gene_rows[0:1, lanes]) * gene_rows[2:3, lanes]
            delta = (two - one * mean) * share_less * gene_rows[3:4, lanes]
            hats.append(hat)
            leans.append(hat - centre)
            floors.append((0.5 * (weight - 1.0) * delta + prior) * inverse)
            deltas.append(delta)
        moves = [None] * GROUPS
        for _ in range(SWEEPS):
            for g in range(GROUPS):
                moves[g] = deltas[g] * leans[g] / (pull + deltas[g])
                deltas[g] = floors[g] + slope * (moves[g] * moves[g])
        for g in range(GROUPS):
            lanes = slice(g * LANES, (g + 1) * LANES)
            scale = lax.rsqrt(deltas[g])
            wide[0, rows, lanes] = scale * gene_rows[2:3, lanes]
            wide[1, rows, lanes] = (hats[g] - moves[g]) * scale
        return carry

    lax.fori_loop(0, BATCHES // block, shrink, 0)
    wide[:, BATCHES:PAD, :] = jnp.zeros((2, PAD - BATCHES, COLS), f32)
    for g in range(2):
        for side in range(2):
            value = wide[side, :, g * PAD : (g + 1) * PAD]
            upper = value.astype(bf16)
            at = slice((2 * g + side) * PAD, (2 * g + side + 1) * PAD)
            pair[0:PAD, at] = upper
            pair[PAD : 2 * PAD, at] = (value - upper.astype(f32)).astype(bf16)

    other = 1 - mh
    partner = my * 2 + other
    to_right, to_left = y_right * 2 + mh, y_left * 2 + mh
    upper_rows, lower_rows = slice(0, CHUNK_TOP), slice(CHUNK_TOP, COMPONENTS)

    def y_at(i):
        step = jnp.where(i == 0, 2, jnp.where(i == 1, 1, jnp.where(i == 2, 3, 0)))
        return lax.rem(my + step, NY)

    def swap(i):
        return remote(part.at[i], part_recv.at[i], d_send.at[i], d_recv.at[i], me_c, partner)

    def y_copy(kind):
        src, dst, to = (
            (role.at[0, upper_rows], y_via_left, to_right),
            (role.at[0, lower_rows], y_via_right, to_left),
            (role.at[1, lower_rows], y_from_left.at[lower_rows], to_right),
            (role.at[2, upper_rows], y_from_right.at[upper_rows], to_left),
            (role.at[1, upper_rows], y_from_left.at[upper_rows], to_right),
            (role.at[2, lower_rows], y_from_right.at[lower_rows], to_left),
        )[kind]
        return remote(src, dst, y_send.at[kind], y_recv.at[kind], me_c, to)

    def adjust(i, carry):
        mine = i >= NY
        place = jnp.where(mine, i - NY, i)
        chunk = jnp.where(mine, mh, other) * NY + y_at(place)
        rows = pl.ds(pl.multiple_of(chunk * STEP, STEP), STEP)
        members = onehot[rows, :]
        members = jnp.concatenate([members, members], axis=1)
        lows = []
        for g in range(2):
            lanes = slice(g * PAD, (g + 1) * PAD)
            found = jnp.dot(members, pair[:, 2 * g * PAD : 2 * (g + 1) * PAD], preferred_element_type=f32)
            grand, gene_sd = gene_rows[0:1, lanes], gene_rows[1:2, lanes]
            standard = (xv[rows, lanes].astype(f32) - grand) * found[:, :PAD] - found[:, PAD:]
            outv[rows, lanes] = (gene_sd * standard + grand).astype(bf16)
            lows.append(standard.astype(bf16))
        part[i] = lax.dot_general(
            loadings_t[...], jnp.concatenate(lows, axis=1), NT, preferred_element_type=f32
        )

        @pl.when(i < NY)
        def _():
            swap(i).start()

        @pl.when(mine)
        def _():
            swap(place).wait_recv()
            role[place] = part[i] + part_recv[place]

        @pl.when(i == NY)
        def _():
            y_copy(0).start()
            y_copy(1).start()

        @pl.when(i == NY + 1)
        def _():
            y_copy(2).start()

        @pl.when(i == NY + 2)
        def _():
            y_copy(3).start()
            y_copy(0).wait_recv()
            role[1, upper_rows] += y_via_left[...]
            y_copy(4).start()
            y_copy(1).wait_recv()
            role[2, lower_rows] += y_via_right[...]
            y_copy(5).start()

        return carry

    lax.fori_loop(0, 2 * NY, adjust, 0)
    for kind in range(2, 6):
        y_copy(kind).wait_recv()
    mine = mh * NY
    final[mine + my] = role[3] + y_from_left[...] + y_from_right[...]

    def y_gather(kind):
        spot, to = (
            (final.at[mine + my, upper_rows], to_right),
            (final.at[mine + my, lower_rows], to_left),
            (final.at[mine + my, lower_rows], to_right),
            (final.at[mine + my, upper_rows], to_left),
            (final.at[mine + y_left, upper_rows], to_right),
            (final.at[mine + y_right, lower_rows], to_left),
        )[kind]
        return remote(spot, spot, y_send.at[6 + kind], y_recv.at[6 + kind], me_c, to)

    def share(i, y):
        spot = final.at[mine + y]
        return remote(spot, spot, d_send.at[NY + i], d_recv.at[NY + i], me_c, partner)

    def store(chunk):
        scores_out[:, pl.ds(pl.multiple_of(chunk * STEP, STEP), STEP)] = final[chunk]

    for kind in range(4):
        y_gather(kind).start()
    share(0, my).start()
    store(mine + my)
    y_gather(0).wait_recv()
    y_gather(4).start()
    y_gather(1).wait_recv()
    y_gather(5).start()
    y_gather(2).wait_recv()
    share(1, y_left).start()
    store(mine + y_left)
    y_gather(3).wait_recv()
    share(2, y_right).start()
    store(mine + y_right)
    y_gather(4).wait_recv()
    y_gather(5).wait_recv()
    share(3, y_opp).start()
    store(mine + y_opp)
    for i, y in enumerate((my, y_left, y_right, y_opp)):
        share(i, y).wait_recv()
        store(other * NY + y)

    for k in range(NZ):
        for kind in range(6):
            rs(kind, k).wait_send()
        for kind in range(4):
            ag(kind, k).wait_send()
        if k < NZ - 1:
            z_copy(k).wait_send()
            g_copy(k).wait_send()
    for r in range(1, 2 * NY):
        terms_over_y(r).wait_send()
    for r in range(1, NX):
        terms_over_x(r).wait_send()
    for i in range(NY):
        swap(i).wait_send()
    for kind in range(6):
        y_copy(kind).wait_send()
        y_gather(kind).wait_send()
    for i, y in enumerate((my, y_left, y_right, y_opp)):
        share(i, y).wait_send()


def body(expression, labels, loadings):
    dma = pltpu.SemaphoreType.DMA
    vmem = pltpu.VMEM
    adjusted, scores_t = pl.pallas_call(
        kernel,
        out_shape=(
            pltpu.VMEM((ROWS, COLS), bf16),
            pltpu.VMEM((COMPONENTS, ROWS), f32),
        ),
        in_specs=[
            pl.BlockSpec(memory_space=vmem),
            pl.BlockSpec(memory_space=pltpu.HBM),
            pl.BlockSpec(memory_space=vmem),
        ],
        out_specs=(pl.BlockSpec(memory_space=vmem), pl.BlockSpec(memory_space=vmem)),
        scratch_shapes=[
            vmem((ROWS, COLS), bf16),
            vmem((ROWS, PAD), bf16),
            vmem((208, COLS), f32),
            vmem((208, COLS), f32),
            vmem((8, PAD), f32),
            vmem((GROUPS, STACK, LANES), f32),
            vmem((NZ, HALF, LANES), f32),
            vmem((NZ, PART - HALF, LANES), f32),
            vmem((NZ, PART, LANES), f32),
            vmem((NZ, PART, LANES), f32),
            vmem((NZ, PART, LANES), f32),
            vmem((NZ, PART, LANES), f32),
            vmem((GROUPS, STACK, LANES), f32),
            vmem((2, 8, PAD), f32),
            vmem((2 * NY, 8, PAD), f32),
            vmem((NX, 8, PAD), f32),
            vmem((7, PAD, LANES), f32),
            vmem((8, COLS), f32),
            vmem((2, PAD, COLS), f32),
            vmem((2 * PAD, 2 * COLS), bf16),
            vmem((2 * NY, COMPONENTS, STEP), f32),
            vmem((NY, COMPONENTS, STEP), f32),
            vmem((NY, COMPONENTS, STEP), f32),
            vmem((CHUNK_TOP, STEP), f32),
            vmem((COMPONENTS - CHUNK_TOP, STEP), f32),
            vmem((COMPONENTS, STEP), f32),
            vmem((COMPONENTS, STEP), f32),
            vmem((2 * NY, COMPONENTS, STEP), f32),
            dma((ROWS // READ,)),
            dma((6, NZ)),
            dma((6, NZ)),
            dma((NZ - 1,)),
            dma((NZ - 1,)),
            dma((NZ - 1,)),
            dma((NZ - 1,)),
            dma((4, NZ)),
            dma((4, NZ)),
            dma((2, 2 * NY)),
            dma((2, 2 * NY)),
            dma((2 * NY,)),
            dma((2 * NY,)),
            dma((12,)),
            dma((12,)),
        ],
        compiler_params=pltpu.CompilerParams(
            collective_id=0, has_side_effects=True, vmem_limit_bytes=56 * 1024 * 1024
        ),
        name="combat",
    )(labels.reshape(ROWS // LANES, LANES), expression, loadings.T)
    return adjusted, scores_t.T


def solution(mesh):
    return jax.shard_map(
        body,
        mesh=mesh,
        in_specs=(P("cells", "genes"), P("cells"), P("genes", None)),
        out_specs=(P("cells", "genes"), P("cells", None)),
        check_vma=False,
    )
```
